512 devices in a mesh: vocab: 64 (over z, y), hid: 4 (over x), tok: 2 (over core).
Axes of the slice: x: 4, y: 8, z: 8, core: 2. Of those that a mesh axis runs over, the one named last changes fastest.
Arguments:
- hidden: bfloat16 [1024, 8192], P('tok', ('hid', 'vocab')), may hold values from -300 to 300
- weight: bfloat16 [8192, 64128], P('hid', 'vocab'), may hold values from -0.1875 to 0.1875
- labels: int32 [1024], P('tok'), may hold values from 0 to 64127
Outputs:
- token_loss: float32 [1024], P('tok')
- mean_loss: float32 [], replicated
The draws below stay inside these ranges and needn't reach their ends.
All inputs are finite; a program needn't handle non-finite values.
Results may differ from the reference program's by a relative error of at most 0.0003.
Values may be sent and summed in bfloat16 or wider, within the bound.
No kernel may reach another device: no remote copies, remote signals or barrier semaphores. Data moves between devices by JAX's collectives and lax.ppermute only.
A program may use at most 64 MiB of HBM per device.

```python
import jax
import jax.numpy as jnp
from jax import lax

D = 8192
V = 64128
TOK_DEV = 512
TOKENS = 1024


def draw_hidden(key, part):
    first, second = jax.random.split(jax.random.fold_in(key, 17), 2)
    values = jax.random.normal(first, (TOKENS, D), jnp.float32)
    scales = jnp.exp(jax.random.uniform(second, (TOKENS, 1), jnp.float32, jnp.log(0.5), jnp.log(4.0)))
    return jnp.clip(values * scales, -300.0, 300.0).astype(jnp.bfloat16)


def with_ends(drawn, rng, smallest, largest):
    index_at = [jax.random.randint(jax.random.fold_in(rng, axis), (), 0, length) for axis, length in enumerate(drawn.shape)]
    main_axis = drawn.shape.index(max(drawn.shape))
    next_to = index_at[:main_axis] + [(index_at[main_axis] + 1) % drawn.shape[main_axis]] + index_at[main_axis + 1:]
    return drawn.at[tuple(index_at)].set(smallest).at[tuple(next_to)].set(largest)


def shard_levels(own_key, dims, shards, low, high):
    def one(dim, parts):
        draws = jax.random.uniform(jax.random.fold_in(jax.random.fold_in(own_key, 6), dim), (parts,), jnp.float32, low / len(shards), high / len(shards))
        return jnp.repeat(jnp.exp(draws), dims[dim] // parts).reshape((-1,) + (1,) * (len(dims) - dim - 1))

    factor_of = one(*shards[0])
    for cut in shards[1:]:
        factor_of = factor_of * one(*cut)
    return factor_of


def centred(rng, shape, spread, limit, shards=(), held_as=jnp.bfloat16):
    result = jax.random.normal(rng, shape, jnp.float32) * spread
    if len(shards) > 0:
        result = shard_levels(rng, shape, shards, -0.22, 0.18) * result
    return jnp.clip(result, min=-limit, max=limit).astype(held_as)


def setup_inputs(seed: int = 0) -> dict:
    streams_of = jax.random.split(jax.random.key(seed), 4)
    return {
        "hidden": draw_hidden(jax.random.fold_in(streams_of[3], 71), 0),
        "weight": centred(streams_of[1], (D, V), (D // 9) ** -0.5, 0.1875, ((0, 4), (1, 64))),
        "labels": with_ends(jax.random.randint(streams_of[2], (TOKENS,), 0, V), jax.random.fold_in(streams_of[2], 1), 0, V - 1).astype(jnp.int32),
    }


def reference(hidden, weight, labels):
    hidden_blocks = hidden.reshape(TOKENS // TOK_DEV, TOK_DEV, D)
    label_blocks = labels.reshape(TOKENS // TOK_DEV, TOK_DEV)

    def one_block(pair):
        rows_in, label_rows = pair
        logits = jnp.dot(rows_in, weight, preferred_element_type=jnp.float32)
        row_top = jnp.max(logits, axis=1)
        lse = row_top + jnp.log(jnp.sum(jnp.exp(logits - row_top[:, None]), axis=1))
        target = jnp.take_along_axis(logits, label_rows[:, None].astype(jnp.int32), axis=1)[:, 0]
        return lse - target

    token_loss = lax.map(one_block, (hidden_blocks, label_blocks)).reshape(TOKENS)
    mean_loss = jnp.sum(token_loss) / TOKENS
    return token_loss, mean_loss
```

```python
import functools

import jax
import jax.numpy as jnp
import numpy as np
from jax import lax
from jax.experimental import pallas as pl
from jax.experimental.pallas import tpu as pltpu
from jax.sharding import Mesh
from jax.sharding import PartitionSpec as P

SENT = jnp.float32
AXES = ("z", "y", "hid", "tok")
MAX_PERMUTES = "8"


def device_ids():
    return np.arange(int(np.prod([lax.axis_size(a) for a in AXES]))).reshape(
        [lax.axis_size(a) for a in AXES]
    )


def even_groups():
    ids = device_ids()
    groups = [
        ids[z::2, y::2, x, core].reshape(-1).tolist()
        for x in range(ids.shape[2])
        for core in range(ids.shape[3])
        for z in range(2)
        for y in range(2)
    ]
    return groups


def shift_pairs(z, y):
    ids = device_ids()
    pairs = []
    for core, sign in enumerate((1, -1)):
        source = ids[:, :, :, core]
        target = np.roll(source, (-sign * z, -sign * y), axis=(0, 1))
        pairs += zip(source.reshape(-1).tolist(), target.reshape(-1).tolist())
    return pairs


def sent_to_all(array, axis, groups=None):
    size = lax.axis_size(axis) if groups is None else len(groups[0])
    copies = jnp.broadcast_to(array, (size, *array.shape))
    return lax.all_to_all(
        copies, axis, split_axis=0, concat_axis=0, axis_index_groups=groups, tiled=True
    )


def gathered_quarters(features):
    own = sent_to_all(features, AXES, even_groups())
    shifts = ((1, 1), (0, 1), (1, 0))
    others = [lax.ppermute(own, AXES, shift_pairs(*shift)) for shift in shifts]
    parity = jnp.stack([lax.axis_index("z") % 2, lax.axis_index("y") % 2]).astype(jnp.int32)
    return [own, *others], ((0, 0), *shifts), parity


def matmul_kernel(parity, *refs, shifts, side, shares, block):
    quarters, weight_ref, out_ref = refs[: len(shifts)], refs[-5], refs[-4]
    rows, held, arrived = refs[-3:]
    width = weight_ref.shape[0]
    starts = range(0, width, block)
    copies = [
        pltpu.make_async_copy(
            weight_ref.at[pl.ds(at, min(block, width - at))],
            held.at[pl.ds(at, min(block, width - at))],
            arrived.at[k],
        )
        for k, at in enumerate(starts)
    ]
    for copy in copies:
        copy.start()
    for quarter, (z, y) in zip(quarters, shifts):
        z = parity[0] ^ z
        y = parity[1] ^ y
        for j in range(quarter.shape[0]):
            rows[(2 * (j // side) + z) * 2 * side + 2 * (j % side) + y] = quarter[j]
    features = rows[...].reshape(-1, rows.shape[-1])
    for at, copy in zip(starts, copies):
        copy.wait()
        tall = min(block, width - at)
        product = jnp.dot(held[at : at + tall], features, preferred_element_type=jnp.float32)
        across = product.shape[1] // shares
        for k in range(shares):
            part = product[:, k * across : (k + 1) * across]
            out_ref[k, at : at + tall] = part.astype(out_ref.dtype)


def partial_logits(quarters, shifts, parity, weight, shares):
    width, depth = weight.shape
    tokens = quarters[0].shape[-1]
    block = 256
    side = lax.axis_size("y") // 2
    return pl.pallas_call(
        functools.partial(matmul_kernel, shifts=shifts, side=side, shares=shares, block=block),
        in_specs=[
            pl.BlockSpec(memory_space=pltpu.SMEM),
            *[pl.BlockSpec(memory_space=pltpu.VMEM) for _ in quarters],
            pl.BlockSpec(memory_space=pl.ANY),
        ],
        out_specs=pl.BlockSpec(memory_space=pltpu.VMEM),
        scratch_shapes=[
            pltpu.VMEM((depth // quarters[0].shape[1], *quarters[0].shape[1:]), weight.dtype),
            pltpu.VMEM((width, depth), weight.dtype),
            pltpu.SemaphoreType.DMA((pl.cdiv(width, block),)),
        ],
        out_shape=jax.ShapeDtypeStruct((shares, width, tokens // shares), SENT),
        compiler_params=pltpu.CompilerParams(vmem_limit_bytes=40 * 2**20),
        name="partial_logits",
    )(parity, *quarters, weight)


def combined(top, summed, target, axis):
    row_top = jnp.max(top, axis=axis)
    scaled = summed * jnp.exp(top - jnp.expand_dims(row_top, axis))
    return row_top, jnp.sum(scaled, axis=axis), jnp.sum(target, axis=axis)


def body(hidden, weight, labels):
    tokens = hidden.shape[0]
    hid = lax.axis_size("hid")
    share = tokens // hid
    width = weight.shape[1]
    quarters, shifts, parity = gathered_quarters(hidden.T)
    blocks = partial_logits(quarters, shifts, parity, weight.T, hid)
    blocks = lax.all_to_all(blocks, "hid", 0, 0, tiled=True)
    logits = jnp.sum(blocks.astype(jnp.float32), axis=0)

    label = lax.dynamic_slice_in_dim(labels, lax.axis_index("hid") * share, share, 0)
    column = label - lax.axis_index(("z", "y")) * width
    hit = lax.broadcasted_iota(jnp.int32, logits.shape, 0) == column[None, :]
    target = jnp.sum(jnp.where(hit, logits, 0.0), axis=0)
    top = jnp.max(logits, axis=0)
    summed = jnp.sum(jnp.exp(logits - top[None, :]), axis=0)

    sent = sent_to_all(jnp.stack([top, summed, target]), ("z", "hid"))
    sent = sent.reshape(lax.axis_size("z"), hid, 3, share)
    found = combined(sent[:, :, 0], sent[:, :, 1], sent[:, :, 2], 0)
    sent = sent_to_all(jnp.stack(found).reshape(3, tokens), ("y", "tok"))
    sent = sent.reshape(lax.axis_size("y"), -1, 3, tokens)
    top, summed, target = combined(sent[:, :, 0], sent[:, :, 1], sent[:, :, 2], 0)
    losses = top + jnp.log(summed) - target
    own = lax.dynamic_index_in_dim(losses, lax.axis_index("tok"), 0, keepdims=False)
    return own, jnp.sum(losses) / losses.size


def solution(mesh):
    finer = Mesh(
        mesh.devices.reshape(8, 8, mesh.shape["hid"], mesh.shape["tok"]),
        AXES,
    )
    in_specs = (P("tok", ("hid", "z", "y")), P("hid", ("z", "y")), P("tok"))
    out_specs = (P("tok"), P())
    return jax.shard_map(body, mesh=finer, in_specs=in_specs, out_specs=out_specs, check_vma=False)
```

```python
import functools

import jax
import jax.numpy as jnp
import numpy as np
from jax import lax
from jax.experimental import pallas as pl
from jax.experimental.pallas import tpu as pltpu
from jax.sharding import Mesh
from jax.sharding import PartitionSpec as P

SENT = jnp.float16
SENT_SCALE = 0.5
AXES = ("z", "y", "hid", "tok")


def device_ids():
    return np.arange(int(np.prod([lax.axis_size(a) for a in AXES]))).reshape(
        [lax.axis_size(a) for a in AXES]
    )


def even_groups():
    ids = device_ids()
    groups = [
        ids[z::2, y::2, x, core].reshape(-1).tolist()
        for x in range(ids.shape[2])
        for core in range(ids.shape[3])
        for z in range(2)
        for y in range(2)
    ]
    return groups


def near_groups():
    ids = device_ids()
    length, width = ids.shape[:2]
    groups = []
    for x in range(ids.shape[2]):
        for core in range(ids.shape[3]):
            for z in range(0, length, 2):
                for y in range(0, width, 2):
                    zs = sorted(((z + core) % length, (z + core + 1) % length), key=lambda n: n % 2)
                    ys = sorted(((y + core) % width, (y + core + 1) % width), key=lambda n: n % 2)
                    groups.append([int(ids[a, b, x, core]) for a in zs for b in ys])
    return groups


def sent_to_all(array, axis, groups=None):
    size = lax.axis_size(axis) if groups is None else len(groups[0])
    copies = jnp.broadcast_to(array, (size, *array.shape))
    return lax.all_to_all(
        copies, axis, split_axis=0, concat_axis=0, axis_index_groups=groups, tiled=True
    )


def gathered_features(features):
    return sent_to_all(sent_to_all(features, AXES, even_groups()), AXES, near_groups())


def matmul_kernel(found, weight_ref, out_ref, rows, *, shares, block):
    width = weight_ref.shape[0]
    side = lax.axis_size("y") // 2
    starts = range(0, width, block)
    for parity in range(found.shape[0]):
        z, y = divmod(parity, 2)
        for j in range(found.shape[1]):
            rows[(2 * (j // side) + z) * 2 * side + 2 * (j % side) + y] = found[parity, j]
    features = rows[...].reshape(-1, rows.shape[-1])
    for at in starts:
        tall = min(block, width - at)
        product = jnp.dot(weight_ref[at : at + tall], features, preferred_element_type=jnp.float32)
        across = product.shape[1] // shares
        for k in range(shares):
            out_ref[k, at : at + tall] = product[:, k * across : (k + 1) * across]


def partial_logits(found, weight, shares):
    width, depth = weight.shape
    own, tokens = found.shape[-2:]
    block = 256
    return pl.pallas_call(
        functools.partial(matmul_kernel, shares=shares, block=block),
        in_specs=[pl.BlockSpec(memory_space=pltpu.VMEM), pl.BlockSpec(memory_space=pltpu.VMEM)],
        out_specs=pl.BlockSpec(memory_space=pltpu.VMEM),
        scratch_shapes=[
            pltpu.VMEM((depth // own, own, tokens), weight.dtype),
        ],
        out_shape=jax.ShapeDtypeStruct((shares, width, tokens // shares), jnp.float32),
        compiler_params=pltpu.CompilerParams(vmem_limit_bytes=40 * 2**20),
        name="partial_logits",
    )(found, weight)


def combined(top, summed, target, axis):
    row_top = jnp.max(top, axis=axis)
    scaled = summed * jnp.exp(top - jnp.expand_dims(row_top, axis))
    return row_top, jnp.sum(scaled, axis=axis), jnp.sum(target, axis=axis)


def body(hidden, weight, labels):
    tokens = hidden.shape[0]
    hid = lax.axis_size("hid")
    share = tokens // hid
    width = weight.shape[1]
    found = gathered_features(hidden.T)
    found = found.reshape(found.shape[0], -1, *found.shape[-2:])
    blocks = partial_logits(found, weight.T, hid)
    blocks = lax.all_to_all((blocks * SENT_SCALE).astype(SENT), "hid", 0, 0, tiled=True)
    logits = jnp.sum(blocks.astype(jnp.float32), axis=0) / SENT_SCALE

    label = lax.dynamic_slice_in_dim(labels, lax.axis_index("hid") * share, share, 0)
    column = label - lax.axis_index(("z", "y")) * width
    hit = lax.broadcasted_iota(jnp.int32, logits.shape, 0) == column[None, :]
    target = jnp.sum(jnp.where(hit, logits, 0.0), axis=0)
    top = jnp.max(logits, axis=0)
    summed = jnp.sum(jnp.exp(logits - top[None, :]), axis=0)

    sent = sent_to_all(jnp.stack([top, summed, target]), ("z", "hid"))
    sent = sent.reshape(lax.axis_size("z"), hid, 3, share)
    found = combined(sent[:, :, 0], sent[:, :, 1], sent[:, :, 2], 0)
    sent = sent_to_all(jnp.stack(found).reshape(3, tokens), ("y", "tok"))
    sent = sent.reshape(lax.axis_size("y"), -1, 3, tokens)
    top, summed, target = combined(sent[:, :, 0], sent[:, :, 1], sent[:, :, 2], 0)
    losses = top + jnp.log(summed) - target
    own = lax.dynamic_index_in_dim(losses, lax.axis_index("tok"), 0, keepdims=False)
    return own, jnp.sum(losses) / losses.size


def solution(mesh):
    finer = Mesh(
        mesh.devices.reshape(8, 8, mesh.shape["hid"], mesh.shape["tok"]),
        AXES,
    )
    in_specs = (P("tok", ("hid", "z", "y")), P("hid", ("z", "y")), P("tok"))
    out_specs = (P("tok"), P())
    return jax.shard_map(body, mesh=finer, in_specs=in_specs, out_specs=out_specs, check_vma=False)
```

```python
import functools

import jax
import jax.numpy as jnp
import numpy as np
from jax import lax
from jax.experimental import pallas as pl
from jax.experimental.pallas import tpu as pltpu
from jax.sharding import Mesh
from jax.sharding import PartitionSpec as P

SENT = jnp.float16
SENT_SCALE = 0.5
AXES = ("z", "y", "hid", "tok")


def device_ids():
    return np.arange(int(np.prod([lax.axis_size(a) for a in AXES]))).reshape(
        [lax.axis_size(a) for a in AXES]
    )


def lines(first):
    ids = device_ids()
    along_z, along_y = (1, 2, 0), (0, 2, 1)
    orders = (along_z, along_y) if first else (along_y, along_z)
    parts = [ids[:, :, :, core].transpose(order) for core, order in enumerate(orders)]
    return [line for part in parts for line in part[..., line_order()].reshape(-1, part.shape[-1]).tolist()]


def line_order():
    size = lax.axis_size("z")
    return [k // 2 if k % 2 == 0 else size - 1 - k // 2 for k in range(size)]


def sent_to_all(array, axis, groups=None):
    size = lax.axis_size(axis) if groups is None else len(groups[0])
    copies = jnp.broadcast_to(array, (size, *array.shape))
    return lax.all_to_all(
        copies, axis, split_axis=0, concat_axis=0, axis_index_groups=groups, tiled=True
    )


def gathered_features(features):
    return sent_to_all(sent_to_all(features, AXES, lines(True)), AXES, lines(False))


def matmul_kernel(found, weight_ref, labels, out_ref, column, core, rows, *, shares, block):
    shard = lax.axis_index("z") * lax.axis_size("y") + lax.axis_index("y")
    column[...] = labels[pl.ds(lax.axis_index("hid"), 1)] - shard * weight_ref.shape[0]
    core[...] = jnp.full(core.shape, lax.axis_index("tok"), jnp.int32)
    width = weight_ref.shape[0]
    side = lax.axis_size("y")
    starts = range(0, width, block)
    first = lax.axis_index("tok") == 0
    for i, far in enumerate(line_order()):
        for j, near in enumerate(line_order()):
            at = jnp.where(first, near * side + far, far * side + near)
            rows[at] = found[i, j]
    features = rows[...].reshape(-1, rows.shape[-1])
    for at in starts:
        tall = min(block, width - at)
        product = jnp.dot(weight_ref[at : at + tall], features, preferred_element_type=jnp.float32)
        across = product.shape[1] // shares
        for k in range(shares):
            out_ref[k, at : at + tall] = product[:, k * across : (k + 1) * across]


def partial_logits(found, weight, labels, shares):
    width, depth = weight.shape
    own, tokens = found.shape[-2:]
    block = 256
    return pl.pallas_call(
        functools.partial(matmul_kernel, shares=shares, block=block),
        in_specs=[pl.BlockSpec(memory_space=pltpu.VMEM)] * 3,
        out_specs=[pl.BlockSpec(memory_space=pltpu.VMEM)] * 3,
        scratch_shapes=[
            pltpu.VMEM((depth // own, own, tokens), weight.dtype),
        ],
        out_shape=[
            jax.ShapeDtypeStruct((shares, width, tokens // shares), jnp.float32),
            jax.ShapeDtypeStruct((1, tokens // shares), jnp.int32),
            jax.ShapeDtypeStruct((1, tokens), jnp.int32),
        ],
        compiler_params=pltpu.CompilerParams(vmem_limit_bytes=40 * 2**20),
        name="partial_logits",
    )(found, weight, labels.reshape(shares, -1))


def log_of_sum(parts, axis):
    top = jnp.max(parts, axis=axis, keepdims=True)
    return jnp.squeeze(top, axis) + jnp.log(jnp.sum(jnp.exp(parts - top), axis=axis))


def combined(parts, axis):
    sums, targets = parts
    return jnp.stack([log_of_sum(sums, axis), jnp.sum(targets, axis=axis)])


def body(hidden, weight, labels):
    tokens = hidden.shape[0]
    hid = lax.axis_size("hid")
    share = tokens // hid
    cores = lax.axis_size("tok")
    found = gathered_features(hidden.T)
    blocks, column, core = partial_logits(found, weight.T, labels, hid)
    blocks = lax.all_to_all((blocks * SENT_SCALE).astype(SENT), "hid", 0, 0, tiled=True)
    logits = jnp.sum(blocks.astype(jnp.float32), axis=0) / SENT_SCALE

    hit = lax.broadcasted_iota(jnp.int32, logits.shape, 0) == column
    target = jnp.sum(jnp.where(hit, logits, 0.0), axis=0)
    sent = sent_to_all(jnp.stack([log_of_sum(logits, 0), target]), ("z", "hid"))
    sent = sent.reshape(-1, hid, 2, share)
    found = combined((sent[:, :, 0], sent[:, :, 1]), 0).reshape(2, tokens)
    sent = sent_to_all(found, ("tok", "y")).reshape(cores, -1, 2, tokens)
    lse, target = combined((sent[:, :, 0], sent[:, :, 1]), 1)
    losses = lse - target
    own = jnp.where(core[0] == 0, losses[0], losses[1])
    return own, jnp.sum(losses) / losses.size


def solution(mesh):
    finer = Mesh(
        mesh.devices.reshape(8, 8, mesh.shape["hid"], mesh.shape["tok"]),
        AXES,
    )
    in_specs = (P("tok", ("hid", "z", "y")), P("hid", ("z", "y")), P("tok"))
    out_specs = (P("tok"), P())
    return jax.shard_map(body, mesh=finer, in_specs=in_specs, out_specs=out_specs, check_vma=False)
```

```python
import functools

import jax
import jax.numpy as jnp
import numpy as np
from jax import lax
from jax.experimental import pallas as pl
from jax.experimental.pallas import tpu as pltpu
from jax.sharding import Mesh
from jax.sharding import PartitionSpec as P

AXES = ("z", "y", "hid", "tok")


def device_ids():
    return np.arange(int(np.prod([lax.axis_size(a) for a in AXES]))).reshape(
        [lax.axis_size(a) for a in AXES]
    )


def lines(first):
    ids = device_ids()
    along_z, along_y = (1, 2, 0), (0, 2, 1)
    orders = (along_z, along_y) if first else (along_y, along_z)
    parts = [ids[:, :, :, core].transpose(order) for core, order in enumerate(orders)]
    return [line for part in parts for line in part[..., line_order()].reshape(-1, part.shape[-1]).tolist()]


def line_order():
    size = lax.axis_size("z")
    return [k // 2 if k % 2 == 0 else size - 1 - k // 2 for k in range(size)]


def sent_to_all(array, axis, groups=None):
    size = lax.axis_size(axis) if groups is None else len(groups[0])
    copies = jnp.broadcast_to(array, (size, *array.shape))
    return lax.all_to_all(
        copies, axis, split_axis=0, concat_axis=0, axis_index_groups=groups, tiled=True
    )


def gathered_features(features):
    return sent_to_all(sent_to_all(features, AXES, lines(True)), AXES, lines(False))


def matmul_kernel(found, weight_ref, labels, out_ref, column, core, rows, *, shares, block):
    shard = lax.axis_index("z") * lax.axis_size("y") + lax.axis_index("y")
    column[...] = labels[pl.ds(lax.axis_index("hid"), 1)] - shard * weight_ref.shape[0]
    core[...] = jnp.full(core.shape, lax.axis_index("tok"), jnp.int32)
    width = weight_ref.shape[0]
    side = lax.axis_size("y")
    starts = range(0, width, block)
    first = lax.axis_index("tok") == 0
    for i, far in enumerate(line_order()):
        for j, near in enumerate(line_order()):
            at = jnp.where(first, near * side + far, far * side + near)
            rows[at] = found[i, j]
    features = rows[...].reshape(-1, rows.shape[-1])
    for at in starts:
        tall = min(block, width - at)
        product = jnp.dot(weight_ref[at : at + tall], features, preferred_element_type=jnp.float32)
        across = product.shape[1] // shares
        for k in range(shares):
            out_ref[k, at : at + tall] = product[:, k * across : (k + 1) * across]


def partial_logits(found, weight, labels, shares):
    width, depth = weight.shape
    own, tokens = found.shape[-2:]
    block = 256
    return pl.pallas_call(
        functools.partial(matmul_kernel, shares=shares, block=block),
        in_specs=[pl.BlockSpec(memory_space=pltpu.VMEM)] * 3,
        out_specs=[pl.BlockSpec(memory_space=pltpu.VMEM)] * 3,
        scratch_shapes=[
            pltpu.VMEM((depth // own, own, tokens), weight.dtype),
        ],
        out_shape=[
            jax.ShapeDtypeStruct((shares, width, tokens // shares), jnp.float32),
            jax.ShapeDtypeStruct((1, tokens // shares), jnp.int32),
            jax.ShapeDtypeStruct((1, tokens), jnp.int32),
        ],
        compiler_params=pltpu.CompilerParams(vmem_limit_bytes=40 * 2**20),
        name="partial_logits",
    )(found, weight, labels.reshape(shares, -1))


def log_of_sum(parts, axis):
    top = jnp.max(parts, axis=axis, keepdims=True)
    return jnp.squeeze(top, axis) + jnp.log(jnp.sum(jnp.exp(parts - top), axis=axis))


def combined(parts, axis):
    sums, targets = parts
    return jnp.stack([log_of_sum(sums, axis), jnp.sum(targets, axis=axis)])


def body(hidden, weight, labels):
    tokens = hidden.shape[0]
    hid = lax.axis_size("hid")
    share = tokens // hid
    cores = lax.axis_size("tok")
    found = gathered_features(hidden.T)
    blocks, column, core = partial_logits(found, weight.T, labels, hid)
    blocks = lax.all_to_all(blocks, "hid", 0, 0, tiled=True)
    logits = jnp.sum(blocks, axis=0)

    hit = lax.broadcasted_iota(jnp.int32, logits.shape, 0) == column
    target = jnp.sum(jnp.where(hit, logits, 0.0), axis=0)
    sent = sent_to_all(jnp.stack([log_of_sum(logits, 0), target]), ("z", "hid"))
    sent = sent.reshape(-1, hid, 2, share)
    found = combined((sent[:, :, 0], sent[:, :, 1]), 0).reshape(2, tokens)
    sent = sent_to_all(found, ("tok", "y")).reshape(cores, -1, 2, tokens)
    lse, target = combined((sent[:, :, 0], sent[:, :, 1]), 1)
    losses = lse - target
    own = jnp.where(core[0] == 0, losses[0], losses[1])
    return own, jnp.sum(losses[0] + losses[1]) / losses.size


def solution(mesh):
    finer = Mesh(
        mesh.devices.reshape(8, 8, mesh.shape["hid"], mesh.shape["tok"]),
        AXES,
    )
    in_specs = (P("tok", ("hid", "z", "y")), P("hid", ("z", "y")), P("tok"))
    out_specs = (P("tok"), P())
    return jax.shard_map(body, mesh=finer, in_specs=in_specs, out_specs=out_specs, check_vma=False)
```

```python
import functools

import jax
import jax.numpy as jnp
import numpy as np
from jax import lax
from jax.experimental import pallas as pl
from jax.experimental.pallas import tpu as pltpu
from jax.sharding import Mesh
from jax.sharding import PartitionSpec as P

SENT = jnp.float16
SENT_SCALE = 0.25
AXES = ("z", "y", "hid", "tok")


def device_ids():
    return np.arange(int(np.prod([lax.axis_size(a) for a in AXES]))).reshape(
        [lax.axis_size(a) for a in AXES]
    )


def lines(first):
    ids = device_ids()
    along_z, along_y = (1, 2, 0), (0, 2, 1)
    orders = (along_z, along_y) if first else (along_y, along_z)
    parts = [ids[:, :, :, core].transpose(order) for core, order in enumerate(orders)]
    return [line for part in parts for line in part[..., line_order()].reshape(-1, part.shape[-1]).tolist()]


def line_order():
    size = lax.axis_size("z")
    return [k // 2 if k % 2 == 0 else size - 1 - k // 2 for k in range(size)]


def sent_to_all(array, axis, groups=None):
    size = lax.axis_size(axis) if groups is None else len(groups[0])
    copies = jnp.broadcast_to(array, (size, *array.shape))
    return lax.all_to_all(
        copies, axis, split_axis=0, concat_axis=0, axis_index_groups=groups, tiled=True
    )


def gathered_features(features):
    return sent_to_all(sent_to_all(features, AXES, lines(True)), AXES, lines(False))


def matmul_kernel(found, weight_ref, labels, out_ref, column, core, rows, *, shares, block):
    shard = lax.axis_index("z") * lax.axis_size("y") + lax.axis_index("y")
    column[...] = labels[pl.ds(lax.axis_index("hid"), 1)] - shard * weight_ref.shape[0]
    core[...] = jnp.full(core.shape, lax.axis_index("tok"), jnp.int32)
    width = weight_ref.shape[0]
    side = lax.axis_size("y")
    starts = range(0, width, block)
    first = lax.axis_index("tok") == 0
    for i, far in enumerate(line_order()):
        for j, near in enumerate(line_order()):
            at = jnp.where(first, near * side + far, far * side + near)
            rows[at] = found[i, j]
    features = rows[...].reshape(-1, rows.shape[-1])
    sums = [0.0] * shares
    for at in starts:
        tall = min(block, width - at)
        product = jnp.dot(weight_ref[at : at + tall], features, preferred_element_type=jnp.float32)
        across = product.shape[1] // shares
        for k in range(shares):
            part = product[:, k * across : (k + 1) * across]
            out_ref[k, at : at + tall] = part
            sums[k] += jnp.sum(part, axis=0, keepdims=True)
    for k in range(shares):
        centre = (sums[k] / width).astype(weight_ref.dtype).astype(jnp.float32)
        out_ref[k, :width] = out_ref[k, :width] - centre
        out_ref[k, width:] = centre


def partial_logits(found, weight, labels, shares):
    width, depth = weight.shape
    own, tokens = found.shape[-2:]
    block = 256
    return pl.pallas_call(
        functools.partial(matmul_kernel, shares=shares, block=block),
        in_specs=[pl.BlockSpec(memory_space=pltpu.VMEM)] * 3,
        out_specs=[pl.BlockSpec(memory_space=pltpu.VMEM)] * 3,
        scratch_shapes=[
            pltpu.VMEM((depth // own, own, tokens), weight.dtype),
        ],
        out_shape=[
            jax.ShapeDtypeStruct((shares, width + 1, tokens // shares), jnp.float32),
            jax.ShapeDtypeStruct((1, tokens // shares), jnp.int32),
            jax.ShapeDtypeStruct((1, tokens), jnp.int32),
        ],
        compiler_params=pltpu.CompilerParams(vmem_limit_bytes=40 * 2**20),
        name="partial_logits",
    )(found, weight, labels.reshape(shares, -1))


def log_of_sum(parts, axis):
    top = jnp.max(parts, axis=axis, keepdims=True)
    return jnp.squeeze(top, axis) + jnp.log(jnp.sum(jnp.exp(parts - top), axis=axis))


def combined(parts, axis):
    sums, targets = parts
    return jnp.stack([log_of_sum(sums, axis), jnp.sum(targets, axis=axis)])


def body(hidden, weight, labels):
    tokens = hidden.shape[0]
    hid = lax.axis_size("hid")
    share = tokens // hid
    cores = lax.axis_size("tok")
    found = gathered_features(hidden.T)
    blocks, column, core = partial_logits(found, weight.T, labels, hid)
    blocks = lax.all_to_all((blocks * SENT_SCALE).astype(SENT), "hid", 0, 0, tiled=True)
    blocks = blocks.astype(jnp.float32)
    logits = jnp.sum(blocks[:, :-1] + blocks[:, -1:], axis=0) / SENT_SCALE

    hit = lax.broadcasted_iota(jnp.int32, logits.shape, 0) == column
    target = jnp.sum(jnp.where(hit, logits, 0.0), axis=0)
    sent = sent_to_all(jnp.stack([log_of_sum(logits, 0), target]), ("z", "hid"))
    sent = sent.reshape(-1, hid, 2, share)
    found = combined((sent[:, :, 0], sent[:, :, 1]), 0).reshape(2, tokens)
    sent = sent_to_all(found, ("tok", "y")).reshape(cores, -1, 2, tokens)
    lse, target = combined((sent[:, :, 0], sent[:, :, 1]), 1)
    losses = lse - target
    own = jnp.where(core[0] == 0, losses[0], losses[1])
    return own, jnp.sum(losses[0] + losses[1]) / losses.size


def solution(mesh):
    finer = Mesh(
        mesh.devices.reshape(8, 8, mesh.shape["hid"], mesh.shape["tok"]),
        AXES,
    )
    in_specs = (P("tok", ("hid", "z", "y")), P("hid", ("z", "y")), P("tok"))
    out_specs = (P("tok"), P())
    return jax.shard_map(body, mesh=finer, in_specs=in_specs, out_specs=out_specs, check_vma=False)
```

```python
import functools

import jax
import jax.numpy as jnp
import numpy as np
from jax import lax
from jax.experimental import pallas as pl
from jax.experimental.pallas import tpu as pltpu
from jax.sharding import Mesh
from jax.sharding import PartitionSpec as P

SENT = jnp.float16
SENT_SCALE = 0.5
AXES = ("z", "y", "hid", "tok")


def device_ids():
    return np.arange(int(np.prod([lax.axis_size(a) for a in AXES]))).reshape(
        [lax.axis_size(a) for a in AXES]
    )


def lines(first):
    ids = device_ids()
    along_z, along_y = (1, 2, 0), (0, 2, 1)
    orders = (along_y, along_z) if first else (along_z, along_y)
    parts = [ids[:, :, :, core].transpose(order) for core, order in enumerate(orders)]
    return [line for part in parts for line in part[..., line_order()].reshape(-1, part.shape[-1]).tolist()]


def line_order():
    size = lax.axis_size("z")
    return [k // 2 if k % 2 == 0 else size - 1 - k // 2 for k in range(size)]


def sent_to_all(array, axis, groups=None):
    size = lax.axis_size(axis) if groups is None else len(groups[0])
    copies = jnp.broadcast_to(array, (size, *array.shape))
    return lax.all_to_all(
        copies, axis, split_axis=0, concat_axis=0, axis_index_groups=groups, tiled=True
    )


def gathered_features(features):
    return sent_to_all(sent_to_all(features, AXES, lines(True)), AXES, lines(False))


def matmul_kernel(found, weight_ref, labels, out_ref, column, core, rows, *, shares, block):
    shard = lax.axis_index("z") * lax.axis_size("y") + lax.axis_index("y")
    column[...] = labels[pl.ds(lax.axis_index("hid"), 1)] - shard * weight_ref.shape[0]
    core[...] = jnp.full(core.shape, lax.axis_index("tok"), jnp.int32)
    width = weight_ref.shape[0]
    side = lax.axis_size("y")
    starts = range(0, width, block)
    first = lax.axis_index("tok") == 1
    for i, far in enumerate(line_order()):
        for j, near in enumerate(line_order()):
            at = jnp.where(first, near * side + far, far * side + near)
            rows[at] = found[i, j]
    features = rows[...].reshape(-1, rows.shape[-1])
    for at in starts:
        tall = min(block, width - at)
        product = jnp.dot(weight_ref[at : at + tall], features, preferred_element_type=jnp.float32)
        across = product.shape[1] // shares
        for k in range(shares):
            out_ref[k, at : at + tall] = product[:, k * across : (k + 1) * across]


def partial_logits(found, weight, labels, shares):
    width, depth = weight.shape
    own, tokens = found.shape[-2:]
    block = 512
    return pl.pallas_call(
        functools.partial(matmul_kernel, shares=shares, block=block),
        in_specs=[pl.BlockSpec(memory_space=pltpu.VMEM)] * 3,
        out_specs=[pl.BlockSpec(memory_space=pltpu.VMEM)] * 3,
        scratch_shapes=[
            pltpu.VMEM((depth // own, own, tokens), weight.dtype),
        ],
        out_shape=[
            jax.ShapeDtypeStruct((shares, width, tokens // shares), jnp.float32),
            jax.ShapeDtypeStruct((1, tokens // shares), jnp.int32),
            jax.ShapeDtypeStruct((1, tokens), jnp.int32),
        ],
        compiler_params=pltpu.CompilerParams(vmem_limit_bytes=40 * 2**20),
        name="partial_logits",
    )(found, weight, labels.reshape(shares, -1))


def log_of_sum(parts, axis):
    top = jnp.max(parts, axis=axis, keepdims=True)
    return jnp.squeeze(top, axis) + jnp.log(jnp.sum(jnp.exp(parts - top), axis=axis))


def combined(parts, axis):
    sums, targets = parts
    return jnp.stack([log_of_sum(sums, axis), jnp.sum(targets, axis=axis)])


def body(hidden, weight, labels):
    tokens = hidden.shape[0]
    hid = lax.axis_size("hid")
    share = tokens // hid
    cores = lax.axis_size("tok")
    found = gathered_features(hidden.T)
    blocks, column, core = partial_logits(found, weight.T, labels, hid)
    blocks = lax.all_to_all((blocks * SENT_SCALE).astype(SENT), "hid", 0, 0, tiled=True)
    logits = jnp.sum(blocks.astype(jnp.float32), axis=0) / SENT_SCALE

    hit = lax.broadcasted_iota(jnp.int32, logits.shape, 0) == column
    target = jnp.sum(jnp.where(hit, logits, 0.0), axis=0)
    sent = sent_to_all(jnp.stack([log_of_sum(logits, 0), target]), ("z", "hid"))
    sent = sent.reshape(-1, hid, 2, share)
    found = combined((sent[:, :, 0], sent[:, :, 1]), 0).reshape(2, tokens)
    sent = sent_to_all(found, ("tok", "y")).reshape(cores, -1, 2, tokens)
    lse, target = combined((sent[:, :, 0], sent[:, :, 1]), 1)
    losses = lse - target
    own = jnp.where(core[0] == 0, losses[0], losses[1])
    return own, jnp.sum(losses[0] + losses[1]) / losses.size


def solution(mesh):
    finer = Mesh(
        mesh.devices.reshape(8, 8, mesh.shape["hid"], mesh.shape["tok"]),
        AXES,
    )
    in_specs = (P("tok", ("hid", "z", "y")), P("hid", ("z", "y")), P("tok"))
    out_specs = (P("tok"), P())
    return jax.shard_map(body, mesh=finer, in_specs=in_specs, out_specs=out_specs, check_vma=False)
```

```python
import functools

import jax
import jax.numpy as jnp
import numpy as np
from jax import lax
from jax.experimental import pallas as pl
from jax.experimental.pallas import tpu as pltpu
from jax.sharding import Mesh
from jax.sharding import PartitionSpec as P

SENT = jnp.float16
SENT_SCALE = 0.5
AXES = ("z", "y", "hid", "tok")


def device_ids():
    return np.arange(int(np.prod([lax.axis_size(a) for a in AXES]))).reshape(
        [lax.axis_size(a) for a in AXES]
    )


def lines(first):
    ids = device_ids()
    along_z, along_y = (1, 2, 0), (0, 2, 1)
    orders = (along_y, along_z) if first else (along_z, along_y)
    parts = [ids[:, :, :, core].transpose(order) for core, order in enumerate(orders)]
    return [line for part in parts for line in part[..., line_order()].reshape(-1, part.shape[-1]).tolist()]


def line_order():
    size = lax.axis_size("z")
    return [k // 2 if k % 2 == 0 else size - 1 - k // 2 for k in range(size)]


def sent_to_all(array, axis, groups=None):
    size = lax.axis_size(axis) if groups is None else len(groups[0])
    copies = jnp.broadcast_to(array, (size, *array.shape))
    return lax.all_to_all(
        copies, axis, split_axis=0, concat_axis=0, axis_index_groups=groups, tiled=True
    )


def gathered_features(features):
    return sent_to_all(sent_to_all(features, AXES, lines(True)), AXES, lines(False))


def matmul_kernel(found, weight_ref, labels, out_ref, column, core, rows, *, shares, block):
    shard = lax.axis_index("z") * lax.axis_size("y") + lax.axis_index("y")
    column[...] = labels[pl.ds(lax.axis_index("hid"), 1)] - shard * weight_ref.shape[0]
    core[...] = jnp.full(core.shape, lax.axis_index("tok"), jnp.int32)
    width = weight_ref.shape[0]
    side = lax.axis_size("y")
    starts = range(0, width, block)
    first = lax.axis_index("tok") == 1
    for i, far in enumerate(line_order()):
        for j, near in enumerate(line_order()):
            at = jnp.where(first, near * side + far, far * side + near)
            rows[at] = found[i, j]
    features = rows[...].reshape(-1, rows.shape[-1])
    for at in starts:
        tall = min(block, width - at)
        product = jnp.dot(weight_ref[at : at + tall], features, preferred_element_type=jnp.float32)
        across = product.shape[1] // shares
        for k in range(shares):
            out_ref[k, at : at + tall] = product[:, k * across : (k + 1) * across]


def partial_logits(found, weight, labels, shares):
    width, depth = weight.shape
    own, tokens = found.shape[-2:]
    block = 256
    return pl.pallas_call(
        functools.partial(matmul_kernel, shares=shares, block=block),
        in_specs=[pl.BlockSpec(memory_space=pltpu.VMEM)] * 3,
        out_specs=[pl.BlockSpec(memory_space=pltpu.VMEM)] * 3,
        scratch_shapes=[
            pltpu.VMEM((depth // own, own, tokens), weight.dtype),
        ],
        out_shape=[
            jax.ShapeDtypeStruct((shares, width, tokens // shares), jnp.float32),
            jax.ShapeDtypeStruct((1, tokens // shares), jnp.int32),
            jax.ShapeDtypeStruct((1, tokens), jnp.int32),
        ],
        compiler_params=pltpu.CompilerParams(vmem_limit_bytes=40 * 2**20),
        name="partial_logits",
    )(found, weight, labels.reshape(shares, -1))


def log_of_sum(parts, axis):
    top = jnp.max(parts, axis=axis, keepdims=True)
    return jnp.squeeze(top, axis) + jnp.log(jnp.sum(jnp.exp(parts - top), axis=axis))


def combined(parts, axis):
    sums, targets = parts
    return jnp.stack([log_of_sum(sums, axis), jnp.sum(targets, axis=axis)])


def body(hidden, weight, labels):
    tokens = hidden.shape[0]
    hid = lax.axis_size("hid")
    share = tokens // hid
    cores = lax.axis_size("tok")
    found = gathered_features(hidden.T)
    blocks, column, core = partial_logits(found, weight.T, labels, hid)
    blocks = lax.all_to_all((blocks * SENT_SCALE).astype(SENT), "hid", 0, 0, tiled=True)
    logits = jnp.sum(blocks.astype(jnp.float32), axis=0) / SENT_SCALE

    hit = lax.broadcasted_iota(jnp.int32, logits.shape, 0) == column
    target = jnp.sum(jnp.where(hit, logits, 0.0), axis=0)
    sent = sent_to_all(jnp.stack([log_of_sum(logits, 0), target]), ("z", "hid"))
    sent = sent.reshape(-1, hid, 2, share)
    found = combined((sent[:, :, 0], sent[:, :, 1]), 0).reshape(2, tokens)
    sent = sent_to_all(found, ("tok", "y")).reshape(cores, -1, 2, tokens)
    lse, target = combined((sent[:, :, 0], sent[:, :, 1]), 1)
    losses = lse - target
    own = jnp.where(core[0] == 0, losses[0], losses[1])
    return own, jnp.sum(losses[0] + losses[1]) / losses.size


def solution(mesh):
    finer = Mesh(
        mesh.devices.reshape(8, 8, mesh.shape["hid"], mesh.shape["tok"]),
        AXES,
    )
    in_specs = (P("tok", ("hid", "z", "y")), P("hid", ("z", "y")), P("tok"))
    out_specs = (P("tok"), P())
    return jax.shard_map(body, mesh=finer, in_specs=in_specs, out_specs=out_specs, check_vma=False)
```
